32 devices in a mesh: groups: 2 (over x), gx: 16 (over z, y, core).
Axes of the slice: x: 2, y: 2, z: 4, core: 2. Of those that a mesh axis runs over, the one named last changes fastest.
Arguments:
- wave_one: float32 [2, 512, 2048], P(None, 'groups', 'gx'), parts along dimension 1, may hold values from -6 to 6
- wave_two: float32 [2, 512, 2048], P(None, 'groups', 'gx'), parts along dimension 1, may hold values from -4.2 to 4.2
- mismatch: float32 [512, 2048], P('groups', 'gx'), parts along dimension 0, may hold values from -1.2 to 1.2
- plate: int32 [16, 64], P('groups', 'gx'), parts along dimension 0, may hold values from 0 to 15
- spot_low: int32 [1024], P('groups'), parts along dimension 0, may hold values from 64 to 255
- spot_high: int32 [1024], P('groups'), parts along dimension 0, may hold values from 256 to 447
- row_gain: float32 [1024], P('groups'), parts along dimension 0, may hold values from 0.5 to 3
- column_gain: float32 [1024], P('groups'), parts along dimension 0, may hold values from 0.5 to 3
Outputs:
- third: float32 [2, 512, 2048], P(None, 'groups', 'gx'), parts along dimension 1
- far_field: float32 [2, 1024, 512], P(None, ('groups', 'gx')), parts along dimension 1
- back_field: float32 [2, 512, 2048], P(None, 'groups', 'gx'), parts along dimension 1
The draws below stay inside these ranges and needn't reach their ends.
There are 2 independent parts, one for each index of `groups`. The reference program is written for one: setup_inputs(seed, part) draws one part's arguments, and reference() takes and returns one part's arrays. A program takes and returns all parts, laid end to end along the dimension named above; each array names one. Nothing has to cross between parts.
All inputs are finite; a program needn't handle non-finite values.
Results may differ from the reference program's by a relative error of at most 0.00017.
Values sent between devices are 32-bit elements; how exact they have to be, the bound alone decides.
No kernel may reach another device: no remote copies, remote signals or barrier semaphores. Data moves between devices by JAX's collectives and lax.ppermute only.
A program may use at most 64 MiB of HBM per device.

```python
import math
import jax
import jax.numpy as jnp
from jax import lax

NY = 256
FFY = 512
FFX = 512
SUBSTEPS = 4
ZOOM = 4
LEVELS = 16
PLATE = 32
NX = 2048
PY = 8
PX = 64


def set_ends(drawn, key, low, high):
    longest = drawn.shape.index(max(drawn.shape))
    spots = []
    for shift in (0, 1):
        where = [jax.random.randint(jax.random.fold_in(key, axis), (), 0, length) for axis, length in enumerate(drawn.shape)]
        where[longest] = (where[longest] + shift) % drawn.shape[longest]
        spots.append(tuple(where))
    return drawn.at[spots[0]].set(low).at[spots[1]].set(high)


def block_scale(stream_key, dims, shards, least, top_value):
    def one(axis_at, shards_of):
        draws = jax.random.uniform(jax.random.fold_in(jax.random.fold_in(stream_key, 6), axis_at), (shards_of,), jnp.float32, least / len(shards), top_value / len(shards))
        return jnp.repeat(jnp.exp(draws), dims[axis_at] // shards_of).reshape((-1,) + (1,) * (len(dims) - axis_at - 1))

    level = one(*shards[0])
    for cut in shards[1:]:
        level = level * one(*cut)
    return level


def scatter_about(key, shape, scale, reach, pieces=(), held_as=jnp.bfloat16):
    array = jax.random.normal(key, shape, jnp.float32) * scale
    if len(pieces) > 0:
        array = block_scale(key, shape, pieces, -0.22, 0.18) * array
    return jnp.clip(array, min=-reach, max=reach).astype(held_as)


def setup_inputs(seed: int = 0, part: int = 0) -> dict:
    splits = jax.random.split(jax.random.key(seed), 9)
    part_splits = jax.random.split(jax.random.fold_in(splits[8], part), 9)
    wave_one = scatter_about(part_splits[0], (2, NY, NX), 1.0, 6.0, ((2, 16),), jnp.float32)
    wave_two = scatter_about(part_splits[1], (2, NY, NX), 0.7, 4.2, ((2, 16),), jnp.float32)
    mismatch = jnp.clip(jax.random.uniform(part_splits[2], (NY, NX), jnp.float32, -1.2, 1.2) * block_scale(part_splits[2], (NY, NX), ((1, 16),), -0.4, 0.0), -1.2, 1.2)
    plate = set_ends(jax.random.randint(part_splits[3], (PY, PX), 0, LEVELS), jax.random.fold_in(part_splits[3], 1), 0, LEVELS - 1).astype(jnp.int32)
    spot_low = set_ends(jax.random.randint(part_splits[4], (FFY,), FFX // 8, FFX // 2), jax.random.fold_in(part_splits[4], 1), FFX // 8, (FFX // 2) - 1).astype(jnp.int32)
    spot_high = set_ends(jax.random.randint(part_splits[5], (FFY,), FFX // 2, 7 * FFX // 8), jax.random.fold_in(part_splits[5], 1), FFX // 2, (7 * FFX // 8) - 1).astype(jnp.int32)
    row_gain = jnp.clip(jnp.exp(jax.random.uniform(part_splits[6], (FFY,), jnp.float32, math.log(0.5), math.log(3.0))), 0.5, 3.0)
    column_gain = jnp.clip(jnp.exp(jax.random.uniform(part_splits[7], (FFX,), jnp.float32, math.log(0.5), math.log(3.0))), 0.5, 3.0)
    return dict(wave_one=wave_one, wave_two=wave_two, mismatch=mismatch, plate=plate, spot_low=spot_low, spot_high=spot_high, row_gain=row_gain, column_gain=column_gain)


DIFFRACT = (0.08, 0.04, 0.027)
WALKOFF = (0.3, -0.8, 0.8)
COUPLE = (0.08, 0.16, 0.24)
FAR_SCALE = 4.0
PRECISE = lax.Precision.HIGHEST

def complex_mul(first_real, first_imaginary, second_real, second_imaginary):
    return (first_real * second_real - first_imaginary * second_imaginary, first_real * second_imaginary + first_imaginary * second_real)

def complex_dot(left_pair, right_pair, contract):

    def product(first, second):
        return lax.dot_general(first, second, (contract, ((), ())), precision=PRECISE, preferred_element_type=jnp.float32)
    real = product(left_pair[0], right_pair[0]) - product(left_pair[1], right_pair[1])
    imaginary = product(left_pair[0], right_pair[1]) + product(left_pair[1], right_pair[0])
    return (real, imaginary)

def increments(fields, mismatch_mid, position):
    middle = fields[:, :, 1:-1]
    left = fields[:, :, :-2]
    right = fields[:, :, 2:]
    blank = jnp.zeros_like(middle[:, :1])
    above = jnp.concatenate([blank, middle[:, :-1]], axis=1)
    below = jnp.concatenate([middle[:, 1:], blank], axis=1)
    laplace = above + below + left + right - 4.0 * middle
    phase = mismatch_mid * position
    cosine = jnp.cos(phase)
    sine_part = jnp.sin(phase)
    term = complex_mul(middle[4], middle[5], middle[2], -middle[3])
    mix_one = complex_mul(term[0], term[1], cosine, -sine_part)
    term = complex_mul(middle[4], middle[5], middle[0], -middle[1])
    mix_two = complex_mul(term[0], term[1], cosine, -sine_part)
    term = complex_mul(middle[0], middle[1], middle[2], middle[3])
    mix_three = complex_mul(term[0], term[1], cosine, sine_part)
    mixing = (mix_one, mix_two, mix_three)
    rates = []
    for wave in range(3):
        spread = DIFFRACT[wave]
        drift = WALKOFF[wave]
        strength = COUPLE[wave]
        for part in range(2):
            channel = 2 * wave + part
            if drift > 0:
                moving = -drift * (middle[channel] - left[channel])
            else:
                moving = -drift * (right[channel] - middle[channel])
            if part == 0:
                rate = -spread * laplace[channel + 1] - strength * mixing[wave][1]
            else:
                rate = spread * laplace[channel - 1] + strength * mixing[wave][0]
            rates.append(rate + moving)
    return jnp.stack(rates)

def substep(fields, mismatch, position):
    padding = ((0, 0), (0, 0), (1, 1))
    first = increments(jnp.pad(fields, padding), mismatch, position)
    trial = fields + first
    second = increments(jnp.pad(trial, padding), mismatch, position + 1.0)
    return fields + 0.5 * (first + second)

def table(positions, count, period):
    frequency = jnp.arange(count, dtype=jnp.int32) - count // 2
    turns = jnp.mod(frequency[:, None] * positions[None, :], period)
    angle = 2.0 * jnp.pi / period * turns.astype(jnp.float32)
    return (jnp.cos(angle), -jnp.sin(angle))

def replace_amplitude(real, imaginary, position, low, high, gain):
    magnitude = jnp.sqrt(real * real + imaginary * imaginary)
    inside = (position >= low) & (position < high)
    factor = gain / jnp.maximum(magnitude, 1.0)
    return (jnp.where(inside, real * factor, real), jnp.where(inside, imaginary * factor, imaginary))

def reference(wave_one, wave_two, mismatch, plate, spot_low, spot_high, row_gain, column_gain):
    fields = jnp.concatenate([wave_one, wave_two, jnp.zeros_like(wave_one)], axis=0)
    for substep_index in range(SUBSTEPS):
        fields = substep(fields, mismatch, float(substep_index))
    third = fields[4:6]
    levels = jnp.repeat(jnp.repeat(plate, PLATE, axis=0), PLATE, axis=1)
    angle = 2.0 * jnp.pi / LEVELS * levels.astype(jnp.float32)
    cosine = jnp.cos(angle)
    sine_part = jnp.sin(angle)
    near = complex_mul(third[0], third[1], cosine, sine_part)
    scale = FAR_SCALE / math.sqrt(NY * NX)
    row_table = table(jnp.arange(NY, dtype=jnp.int32) - NY // 2, FFY, ZOOM * NY)
    column_table = table(jnp.arange(NX, dtype=jnp.int32) - NX // 2, FFX, FFX)
    rows_done = complex_dot(row_table, near, ((1,), (0,)))
    spectrum = complex_dot(rows_done, column_table, ((1,), (1,)))
    far_real = scale * spectrum[0]
    far_imaginary = scale * spectrum[1]
    position = jnp.arange(FFX, dtype=jnp.int32)[None, :]
    gain = row_gain[:, None] * column_gain[None, :]
    replaced = replace_amplitude(far_real, far_imaginary, position, spot_low[:, None], spot_high[:, None], gain)
    conj_column = (column_table[0], -column_table[1])
    conj_row = (row_table[0], -row_table[1])
    across = complex_dot(replaced, conj_column, ((1,), (0,)))
    summed = complex_dot(conj_row, across, ((0,), (0,)))
    back = complex_mul(scale * summed[0], scale * summed[1], cosine, -sine_part)
    return (third, jnp.stack([far_real, far_imaginary]), jnp.stack([back[0], back[1]]))
```

```python
import functools
import math

import jax
import jax.numpy as jnp
import ml_dtypes
import numpy as np
from jax import lax
from jax.experimental import pallas as pl
from jax.experimental.pallas import tpu as pltpu
from jax.sharding import PartitionSpec as P

SUBSTEPS = 4
ZOOM = 4
LEVELS = 16
PLATE = 32

DIFFRACT = (0.08, 0.04, 0.027)
WALKOFF = (0.3, -0.8, 0.8)
COUPLE = (0.08, 0.16, 0.24)
FAR_SCALE = 4.0

UNITS = tuple(
    math.sqrt(COUPLE[j] / (COUPLE[0] * COUPLE[1] * COUPLE[2])) for j in range(3)
)
HALO = 2 * SUBSTEPS
TILE = 8
LANES = 128
F32 = jnp.float32
BF16 = jnp.bfloat16


def split_table(table):
    high = table.astype(np.float32).astype(ml_dtypes.bfloat16)
    low = (table - high.astype(np.float64)).astype(np.float32).astype(ml_dtypes.bfloat16)
    return high, low


def row_tables(rows, far_rows, scale):
    u = np.arange(far_rows, dtype=np.int64) - far_rows // 2
    y = np.arange(rows, dtype=np.int64) - rows // 2
    period = ZOOM * rows
    angle = 2.0 * np.pi / period * np.mod(u[:, None] * y[None, :], period)
    real, imaginary = scale * np.cos(angle), -scale * np.sin(angle)
    forward = np.concatenate([real, imaginary], axis=1)
    backward = np.concatenate([real.T, imaginary.T], axis=1)
    return split_table(forward), split_table(backward)


def column_tables(far_columns):
    v = np.arange(far_columns, dtype=np.int64)
    angle = 2.0 * np.pi / far_columns * np.mod(v[:, None] * v[None, :], far_columns)
    return split_table(np.concatenate([np.cos(angle), np.sin(angle)], axis=1))


def split(value):
    high = value.astype(BF16)
    low = (value - high.astype(F32)).astype(BF16)
    return high, low


def dot(left, right):
    return jnp.dot(left, right, preferred_element_type=F32)


def plate_phase(levels):
    count, across = levels.shape
    block = lax.broadcasted_iota(jnp.int32, (count, across * PLATE), 1) // PLATE
    level = jnp.zeros((count, across * PLATE), F32)
    for b in range(across):
        level = jnp.where(block == b, levels[:, b : b + 1].astype(F32), level)
    angle = (2.0 * math.pi / LEVELS) * level
    return jnp.cos(angle), jnp.sin(angle)


def edges_kernel(one_ref, two_ref, mismatch_ref, turned_ref, near_ref, far_ref):
    halves = one_ref.shape[1] // LANES
    width = one_ref.shape[2]
    even = lax.rem(lax.axis_index("gx"), 2) == 0
    for c in range(5):
        for h in range(halves):
            rows = pl.ds(h * LANES, LANES)
            if c < 2:
                block = one_ref[c, rows, :] * (1.0 / UNITS[0])
            elif c < 4:
                block = two_ref[c - 2, rows, :] * (1.0 / UNITS[1])
            else:
                block = mismatch_ref[rows, :]
            block = block.T
            turned_ref[c, h] = block
            first, last = block[:HALO], block[width - HALO :]
            near_ref[c, h] = jnp.where(even, last, first)
            far_ref[c, h] = jnp.where(even, first, last)


def sine_pair(angle):
    q = angle * angle
    sine = jnp.full_like(q, 1.0 / math.factorial(15) * -1.0)
    cosine = jnp.full_like(q, 1.0 / math.factorial(16))
    for k in (13, 11, 9, 7, 5, 3, 1):
        sine = sine * q + (-1.0) ** (k // 2) / math.factorial(k)
    for k in (14, 12, 10, 8, 6, 4, 2, 0):
        cosine = cosine * q + (-1.0) ** (k // 2) / math.factorial(k)
    return cosine, sine * angle


def cmul(a, b):
    return a[0] * b[0] - a[1] * b[1], a[0] * b[1] + a[1] * b[0]


def cmul_conj(a, b):
    return a[0] * b[0] + a[1] * b[1], a[1] * b[0] - a[0] * b[1]


def advance(source, row, halves, turn, start, waves):
    lane = lax.broadcasted_iota(jnp.int32, (TILE, LANES), 1)
    used = range(4) if start else range(6)
    mid = [[source[c, h, pl.ds(row, TILE), :] for h in range(halves)] for c in used]
    linear = {}
    for wave in waves:
        if start and wave == 2:
            continue
        side = -1 if WALKOFF[wave] > 0 else 1
        drift, spread = abs(WALKOFF[wave]), DIFFRACT[wave]
        for part in range(2):
            c = 2 * wave + part
            up = [pltpu.roll(m, 1, 1) for m in mid[c]]
            down = [pltpu.roll(m, LANES - 1, 1) for m in mid[c]]
            for h in range(halves):
                above = jnp.where(lane == 0, up[h - 1] if h else 0.0, up[h])
                beyond = down[h + 1] if h + 1 < halves else 0.0
                below = jnp.where(lane == LANES - 1, beyond, down[h])
                left = source[c, h, pl.ds(row - 1, TILE), :]
                right = source[c, h, pl.ds(row + 1, TILE), :]
                around = (above + below) + (left + right)
                m = mid[c][h]
                bend = spread * around - (4.0 * spread) * m
                move = (1.0 - drift) * m + drift * (left if side < 0 else right)
                linear[c, h] = (bend, move)
    out = {}
    for h in range(halves):
        a1, a2 = (mid[0][h], mid[1][h]), (mid[2][h], mid[3][h])
        mixes = {}
        if start:
            mixes[2] = cmul(a1, a2)
        else:
            a3 = (mid[4][h], mid[5][h])
            phase = turn(h)
            if 0 in waves:
                back = cmul_conj(a3, phase) if phase is not None else a3
                mixes[0] = cmul_conj(back, a2)
                mixes[1] = cmul_conj(back, a1)
            ahead = cmul(a1, phase) if phase is not None else a1
            mixes[2] = cmul(ahead, a2)
        for wave in waves:
            real, imaginary = 2 * wave, 2 * wave + 1
            mix = mixes.get(wave)
            if (real, h) not in linear:
                out[real, h], out[imaginary, h] = -mix[1], mix[0]
                continue
            real_part = linear[real, h][1] - linear[imaginary, h][0]
            imaginary_part = linear[imaginary, h][1] + linear[real, h][0]
            if mix is not None:
                real_part = real_part - mix[1]
                imaginary_part = imaginary_part + mix[0]
            out[real, h], out[imaginary, h] = real_part, imaginary_part
    return out


def crystal_kernel(
    turned_ref, near_ref, far_ref, plate_ref, high_ref, low_ref,
    third_ref, sent_ref,
    field, trial, angles, result,
):
    halves, width = turned_ref.shape[1], turned_ref.shape[2]
    devices = sent_ref.shape[0]
    index = lax.axis_index("gx")
    even = lax.rem(index, 2) == 0
    tiles = width // TILE + 2
    begin = 2 * TILE
    keep_first = jnp.where(index > 0, 1.0, 0.0).astype(F32)
    keep_last = jnp.where(index < devices - 1, 1.0, 0.0).astype(F32)

    zero = jnp.zeros((TILE, LANES), F32)
    for h in range(halves):
        for c in range(6):
            for at in (0, (tiles + 1) * TILE):
                field[c, h, pl.ds(at, TILE), :] = zero
                trial[c, h, pl.ds(at, TILE), :] = zero
        for c in range(4):
            field[c, h, pl.ds(begin, width), :] = turned_ref[c, h]
            a, b = near_ref[c, h], far_ref[c, h]
            field[c, h, pl.ds(TILE, TILE), :] = jnp.where(even, b, a) * keep_first
            field[c, h, pl.ds(begin + width, TILE), :] = jnp.where(even, a, b) * keep_last

    def store_angles(h, row, value):
        c1, s1 = sine_pair(value)
        one = (c1, s1)
        two = (c1 * c1 - s1 * s1, 2.0 * c1 * s1)
        three = cmul(one, two)
        four = (two[0] * two[0] - two[1] * two[1], 2.0 * two[0] * two[1])
        for z, pair in enumerate((one, two, three, four)):
            angles[2 * z, h, pl.ds(row, TILE), :] = pair[0]
            angles[2 * z + 1, h, pl.ds(row, TILE), :] = pair[1]

    for h in range(halves):
        a, b = near_ref[4, h], far_ref[4, h]
        store_angles(h, TILE, jnp.where(even, b, a))
        store_angles(h, begin + width, jnp.where(even, a, b))

    def angle_body(t, carry):
        for h in range(halves):
            row = pl.multiple_of(t * TILE, TILE)
            store_angles(h, pl.multiple_of(row + begin, TILE), turned_ref[4, h, pl.ds(row, TILE), :])
        return carry

    lax.fori_loop(0, width // TILE, angle_body, 0, unroll=2)

    def turn_at(z, row):
        def turn(h):
            if z == 0:
                return None
            return tuple(angles[2 * (z - 1) + k, h, pl.ds(row, TILE), :] for k in range(2))

        return turn

    def first_half(step, row, keep):
        out = advance(field, row, halves, turn_at(step, row), step == 0, range(3))
        for (c, h), value in out.items():
            trial[c, h, pl.ds(row, TILE), :] = value if keep is None else value * keep

    def second_half(step, row, keep):
        last = step == SUBSTEPS - 1
        waves = (2,) if last else range(3)
        out = advance(trial, row, halves, turn_at(step + 1, row), False, waves)
        for (c, h), value in out.items():
            if step == 0 and c >= 4:
                value = 0.5 * value
            else:
                value = 0.5 * (field[c, h, pl.ds(row, TILE), :] + value)
            if last:
                at = pl.multiple_of(row - begin, TILE)
                result[c - 4, h, pl.ds(at, TILE), :] = value * UNITS[2]
            else:
                field[c, h, pl.ds(row, TILE), :] = value if keep is None else value * keep

    def sweep(half, step, edges):
        if edges:
            half(step, TILE, keep_first)
            half(step, tiles * TILE, keep_last)

        def body(t, carry):
            half(step, pl.multiple_of(begin + t * TILE, TILE), None)
            return carry

        lax.fori_loop(0, width // TILE, body, 0, unroll=2)

    for step in range(SUBSTEPS):
        sweep(first_half, step, True)
        sweep(second_half, step, step < SUBSTEPS - 1)

    cosine, sine_part = plate_phase(plate_ref[...])
    parts = [[], []]
    for h in range(halves):
        blocks = [result[p, h].T for p in range(2)]
        for p in range(2):
            third_ref[p, pl.ds(h * LANES, LANES), :] = blocks[p]
        for k in range(LANES // PLATE):
            at = h * (LANES // PLATE) + k
            turn = (cosine[at : at + 1], sine_part[at : at + 1])
            piece = [b[k * PLATE : (k + 1) * PLATE] for b in blocks]
            product = cmul(piece, turn)
            for p in range(2):
                parts[p].append(product[p])
    real, imaginary = (jnp.concatenate(p, axis=0) for p in parts)
    data = jnp.concatenate(
        [jnp.concatenate([real, imaginary], axis=1), jnp.concatenate([-imaginary, real], axis=1)],
        axis=0,
    )
    high, low = split(data)
    spectrum = dot(high_ref[...], high) + (dot(high_ref[...], low) + dot(low_ref[...], high))
    share = spectrum.shape[0] // devices
    for d in range(devices):
        for p in range(2):
            sent_ref[d, p] = spectrum[d * share : (d + 1) * share, p * width : (p + 1) * width]


def spot_kernel(
    got_ref, low_ref, high_ref, row_ref, column_ref, table_high_ref, table_low_ref,
    far_ref, sent_ref,
):
    devices, _, share, width = got_ref.shape
    columns = column_ref.shape[1]
    classes = columns // width
    first = lax.axis_index("gx") * share

    folded = []
    for p in range(2):
        pieces = []
        for k in range(classes):
            terms = [got_ref[d, p] for d in range(k, devices, classes)]
            while len(terms) > 1:
                terms = [sum(terms[i : i + 2]) for i in range(0, len(terms), 2)]
            pieces.append(terms[0])
        folded.append(jnp.concatenate(pieces, axis=1))
    position = lax.broadcasted_iota(jnp.int32, (2 * share, columns), 1)
    parity = (1 - 2 * lax.rem(position, 2)).astype(F32)

    def transform(stacked):
        high, low = split(stacked)
        both = dot(jnp.concatenate([high, low], axis=0), table_high_ref[...])
        total = both[: 2 * share] + (both[2 * share :] + dot(high, table_low_ref[...]))
        return total[:, :columns], total[:, columns:]

    cosines, sines = transform(jnp.concatenate(folded, axis=0) * parity)
    far_real = cosines[:share] + sines[share:]
    far_imaginary = cosines[share:] - sines[:share]
    far_ref[0] = far_real
    far_ref[1] = far_imaginary

    rows = low_ref.shape[1]
    own = lax.broadcasted_iota(jnp.int32, (share, rows), 1) == first + lax.broadcasted_iota(
        jnp.int32, (share, rows), 0
    )

    def own_rows(ref):
        value = jnp.where(own, ref[...].astype(F32), 0.0)
        return jnp.sum(value, axis=1, keepdims=True)

    spot = lax.broadcasted_iota(jnp.int32, (share, columns), 1).astype(F32)
    inside = (spot >= own_rows(low_ref)) & (spot < own_rows(high_ref))
    gain = own_rows(row_ref) * column_ref[...]
    power = far_real * far_real + far_imaginary * far_imaginary
    factor = jnp.where(inside, gain * lax.rsqrt(jnp.maximum(power, 1.0)), 1.0)
    replaced = jnp.concatenate([far_real * factor, far_imaginary * factor], axis=0)
    cosines, sines = transform(replaced)
    parity = parity[:share]
    across = (
        (cosines[:share] - sines[share:]) * parity,
        (cosines[share:] + sines[:share]) * parity,
    )
    for d in range(devices):
        k = d % classes
        for p in range(2):
            sent_ref[d, p] = across[p][:, k * width : (k + 1) * width]


def back_kernel(got_ref, plate_ref, high_ref, low_ref, back_ref):
    devices, _, share, width = got_ref.shape
    real = got_ref[:, 0].reshape(devices * share, width)
    imaginary = got_ref[:, 1].reshape(devices * share, width)
    data = jnp.concatenate(
        [jnp.concatenate([real, imaginary], axis=1), jnp.concatenate([imaginary, -real], axis=1)],
        axis=0,
    )
    high, low = split(data)
    total = dot(high_ref[...], high) + (dot(high_ref[...], low) + dot(low_ref[...], high))
    cosine, sine_part = plate_phase(plate_ref[...])
    for k in range(total.shape[0] // PLATE):
        rows = slice(k * PLATE, (k + 1) * PLATE)
        piece = (total[rows, :width], total[rows, width:])
        turn = (cosine[k : k + 1], sine_part[k : k + 1])
        product = cmul_conj(piece, turn)
        for p in range(2):
            back_ref[p, rows, :] = product[p]


def shape(*dims):
    return jax.ShapeDtypeStruct(dims, F32)


def local(wave_one, wave_two, mismatch, plate, spot_low, spot_high, row_gain, column_gain):
    devices = lax.axis_size("gx")
    rows, width = wave_one.shape[1:]
    far_rows, far_columns = row_gain.shape[0], column_gain.shape[0]
    whole_width = width * devices
    halves = rows // LANES
    share = far_rows // devices
    assert rows % LANES == 0 and width == LANES
    assert far_columns % width == 0 and devices % (far_columns // width) == 0
    assert (whole_width // 2) % far_columns == 0 and devices % 2 == 0
    scale = FAR_SCALE / math.sqrt(rows * whole_width)
    forward, backward = row_tables(rows, far_rows, scale)
    columns = column_tables(far_columns)

    strip = shape(5, halves, HALO, LANES)
    turned, near, far = pl.pallas_call(
        edges_kernel, out_shape=(shape(5, halves, width, LANES), strip, strip), name="edges"
    )(wave_one, wave_two, mismatch)
    near = lax.ppermute(near, "gx", [(i, i ^ 1) for i in range(devices)])
    pairs = [(i, i + 1) for i in range(1, devices - 1, 2)]
    far = lax.ppermute(far, "gx", pairs + [(j, i) for i, j in pairs])

    length = width + 4 * TILE
    third, sent = pl.pallas_call(
        crystal_kernel,
        out_shape=(shape(2, rows, width), shape(devices, 2, share, width)),
        scratch_shapes=[
            pltpu.VMEM((6, halves, length, LANES), F32),
            pltpu.VMEM((6, halves, length, LANES), F32),
            pltpu.VMEM((2 * SUBSTEPS, halves, length, LANES), F32),
            pltpu.VMEM((2, halves, width, LANES), F32),
        ],
        name="crystal",
    )(turned, near, far, plate, *forward)
    got = lax.all_to_all(sent, "gx", 0, 0, tiled=True)
    far_field, sent = pl.pallas_call(
        spot_kernel,
        out_shape=(shape(2, share, far_columns), shape(devices, 2, share, width)),
        name="spot",
    )(
        got,
        spot_low.reshape(1, far_rows),
        spot_high.reshape(1, far_rows),
        row_gain.reshape(1, far_rows),
        column_gain.reshape(1, far_columns),
        *columns,
    )
    got = lax.all_to_all(sent, "gx", 0, 0, tiled=True)
    back = pl.pallas_call(back_kernel, out_shape=shape(2, rows, width), name="back")(
        got, plate, *backward
    )
    return third, far_field, back


def solution(mesh):
    return jax.shard_map(
        local,
        mesh=mesh,
        in_specs=(
            P(None, "groups", "gx"),
            P(None, "groups", "gx"),
            P("groups", "gx"),
            P("groups", "gx"),
            P("groups"),
            P("groups"),
            P("groups"),
            P("groups"),
        ),
        out_specs=(
            P(None, "groups", "gx"),
            P(None, ("groups", "gx"), None),
            P(None, "groups", "gx"),
        ),
        check_vma=False,
    )
```

```python
import functools
import math

import jax
import jax.numpy as jnp
import ml_dtypes
import numpy as np
from jax import lax
from jax.experimental import pallas as pl
from jax.experimental.pallas import tpu as pltpu
from jax.sharding import PartitionSpec as P

SUBSTEPS = 4
ZOOM = 4
LEVELS = 16
PLATE = 32

DIFFRACT = (0.08, 0.04, 0.027)
WALKOFF = (0.3, -0.8, 0.8)
COUPLE = (0.08, 0.16, 0.24)
FAR_SCALE = 4.0

UNITS = tuple(
    math.sqrt(COUPLE[j] / (COUPLE[0] * COUPLE[1] * COUPLE[2])) for j in range(3)
)
HALO = 2 * SUBSTEPS
TILE = 8
GROUPS = 1
LANES = 128
F32 = jnp.float32
BF16 = jnp.bfloat16


def split_table(table):
    high = table.astype(np.float32).astype(ml_dtypes.bfloat16)
    low = (table - high.astype(np.float64)).astype(np.float32).astype(ml_dtypes.bfloat16)
    return high, low


def row_tables(rows, far_rows, scale):
    u = np.arange(far_rows, dtype=np.int64) - far_rows // 2
    y = np.arange(rows, dtype=np.int64) - rows // 2
    period = ZOOM * rows
    angle = 2.0 * np.pi / period * np.mod(u[:, None] * y[None, :], period)
    real, imaginary = scale * np.cos(angle), -scale * np.sin(angle)
    halves = rows // LANES
    order = np.arange(rows).reshape(LANES, halves).T.reshape(-1)
    forward = np.concatenate([real[:, order], imaginary[:, order]], axis=1)
    backward = np.concatenate([real.T, imaginary.T], axis=1)
    return split_table(forward), split_table(backward)


def column_tables(far_columns):
    v = np.arange(far_columns, dtype=np.int64)
    angle = 2.0 * np.pi / far_columns * np.mod(v[:, None] * v[None, :], far_columns)
    return split_table(np.concatenate([np.cos(angle), np.sin(angle)], axis=1))


def split(value):
    high = value.astype(BF16)
    low = (value - high.astype(F32)).astype(BF16)
    return high, low


def dot(left, right):
    return jnp.dot(left, right, preferred_element_type=F32)


def plate_phase(levels):
    count, across = levels.shape
    block = lax.broadcasted_iota(jnp.int32, (count, across * PLATE), 1) // PLATE
    level = jnp.zeros((count, across * PLATE), F32)
    for b in range(across):
        level = jnp.where(block == b, levels[:, b : b + 1].astype(F32), level)
    angle = (2.0 * math.pi / LEVELS) * level
    return jnp.cos(angle), jnp.sin(angle)


def start_copies(sources, targets, sems):
    copies = [
        pltpu.make_async_copy(a, b, sems.at[i]) for i, (a, b) in enumerate(zip(sources, targets))
    ]
    for copy in copies:
        copy.start()
    return copies


def edges_kernel(
    one_hbm, two_hbm, mismatch_hbm, turned_ref, near_ref, far_ref,
    one_ref, two_ref, mismatch_ref, sems,
):
    halves = one_ref.shape[1] // LANES
    width = one_ref.shape[2]
    copies = start_copies(
        (one_hbm, two_hbm, mismatch_hbm), (one_ref, two_ref, mismatch_ref), sems
    )
    even = lax.rem(lax.axis_index("gx"), 2) == 0
    for c in range(5):
        if c % 2 == 0:
            copies[c // 2].wait()
        for h in range(halves):
            rows = pl.ds(h, LANES, stride=halves)
            if c < 2:
                block = one_ref[c, rows, :] * (1.0 / UNITS[0])
            elif c < 4:
                block = two_ref[c - 2, rows, :] * (1.0 / UNITS[1])
            else:
                block = mismatch_ref[rows, :]
            block = block.T
            turned_ref[c, h] = block
            first, last = block[:HALO], block[width - HALO :]
            near_ref[c, h] = jnp.where(even, last, first)
            far_ref[c, h] = jnp.where(even, first, last)


def sine_pair(angle):
    q = angle * angle
    sine = (1.0 / math.factorial(13)) * q - 1.0 / math.factorial(11)
    cosine = (-1.0 / math.factorial(14)) * q + 1.0 / math.factorial(12)
    for k in (9, 7, 5, 3, 1):
        sine = sine * q + (-1.0) ** (k // 2) / math.factorial(k)
    for k in (10, 8, 6, 4, 2, 0):
        cosine = cosine * q + (-1.0) ** (k // 2) / math.factorial(k)
    return cosine, sine * angle


def cmul(a, b):
    return a[0] * b[0] - a[1] * b[1], a[0] * b[1] + a[1] * b[0]


def cmul_conj(a, b):
    return a[0] * b[0] + a[1] * b[1], a[1] * b[0] - a[0] * b[1]


def advance(source, row, halves, turn, start, waves):
    lane = lax.broadcasted_iota(jnp.int32, (TILE, LANES), 1)
    used = range(4) if start else range(6)
    mid = [[source[c, h, pl.ds(row, TILE), :] for h in range(halves)] for c in used]
    linear = {}
    for wave in waves:
        if start and wave == 2:
            continue
        side = -1 if WALKOFF[wave] > 0 else 1
        drift, spread = abs(WALKOFF[wave]), DIFFRACT[wave]
        for part in range(2):
            c = 2 * wave + part
            wrap = jnp.where(lane == 0, 0.0, pltpu.roll(mid[c][-1], 1, 1))
            over = jnp.where(lane == LANES - 1, 0.0, pltpu.roll(mid[c][0], LANES - 1, 1))
            for h in range(halves):
                above = mid[c][h - 1] if h else wrap
                below = mid[c][h + 1] if h + 1 < halves else over
                left = source[c, h, pl.ds(row - 1, TILE), :]
                right = source[c, h, pl.ds(row + 1, TILE), :]
                around = (above + below) + (left + right)
                m = mid[c][h]
                bend = spread * around - (4.0 * spread) * m
                move = (1.0 - drift) * m + drift * (left if side < 0 else right)
                linear[c, h] = (bend, move)
    out = {}
    for h in range(halves):
        a1, a2 = (mid[0][h], mid[1][h]), (mid[2][h], mid[3][h])
        mixes = {}
        if start:
            mixes[2] = cmul(a1, a2)
        else:
            a3 = (mid[4][h], mid[5][h])
            phase = turn(h)
            if 0 in waves:
                back = cmul_conj(a3, phase) if phase is not None else a3
                mixes[0] = cmul_conj(back, a2)
                mixes[1] = cmul_conj(back, a1)
            ahead = cmul(a1, phase) if phase is not None else a1
            mixes[2] = cmul(ahead, a2)
        for wave in waves:
            real, imaginary = 2 * wave, 2 * wave + 1
            mix = mixes.get(wave)
            if (real, h) not in linear:
                out[real, h], out[imaginary, h] = -mix[1], mix[0]
                continue
            real_part = linear[real, h][1] - linear[imaginary, h][0]
            imaginary_part = linear[imaginary, h][1] + linear[real, h][0]
            if mix is not None:
                real_part = real_part - mix[1]
                imaginary_part = imaginary_part + mix[0]
            out[real, h], out[imaginary, h] = real_part, imaginary_part
    return out


def crystal_kernel(
    turned_ref, near_ref, far_ref, plate_ref, high_hbm, low_hbm, *rest
):
    spots, (third_ref, sent_ref), rest = rest[:4], rest[4:6], rest[6:]
    kept, (field, trial, angles, result, high_ref, low_ref, sems) = rest[:4], rest[4:]
    copies = start_copies((high_hbm, low_hbm, *spots), (high_ref, low_ref, *kept), sems)
    halves, width = turned_ref.shape[1], turned_ref.shape[2]
    devices = sent_ref.shape[0]
    index = lax.axis_index("gx")
    even = lax.rem(index, 2) == 0
    tiles = width // TILE + 2
    begin = 2 * TILE
    keep_first = jnp.where(index > 0, 1.0, 0.0).astype(F32)
    keep_last = jnp.where(index < devices - 1, 1.0, 0.0).astype(F32)

    zero = jnp.zeros((TILE, LANES), F32)
    for h in range(halves):
        for c in range(6):
            for at in (0, (tiles + 1) * TILE):
                field[c, h, pl.ds(at, TILE), :] = zero
                trial[c, h, pl.ds(at, TILE), :] = zero
        for c in range(4):
            field[c, h, pl.ds(begin, width), :] = turned_ref[c, h]
            a, b = near_ref[c, h], far_ref[c, h]
            field[c, h, pl.ds(TILE, TILE), :] = jnp.where(even, b, a) * keep_first
            field[c, h, pl.ds(begin + width, TILE), :] = jnp.where(even, a, b) * keep_last

    def store_angles(h, row, value):
        c1, s1 = sine_pair(value)
        one = (c1, s1)
        two = (c1 * c1 - s1 * s1, 2.0 * c1 * s1)
        three = cmul(one, two)
        four = (two[0] * two[0] - two[1] * two[1], 2.0 * two[0] * two[1])
        for z, pair in enumerate((one, two, three, four)):
            for late in range(2 if z < 3 else 1):
                at, unit = 4 * z + 2 * late, 0.5 ** (z + late)
                for k in range(2):
                    angles[at + k, h, pl.ds(row, TILE), :] = unit * pair[k]

    for h in range(halves):
        a, b = near_ref[4, h], far_ref[4, h]
        store_angles(h, TILE, jnp.where(even, b, a))
        store_angles(h, begin + width, jnp.where(even, a, b))

    def angle_body(t, carry):
        for h in range(halves):
            row = pl.multiple_of(t * TILE, TILE)
            store_angles(h, pl.multiple_of(row + begin, TILE), turned_ref[4, h, pl.ds(row, TILE), :])
        return carry

    lax.fori_loop(0, width // TILE, angle_body, 0, unroll=2)

    def turn_at(z, late, row):
        def turn(h):
            if z == 0:
                return None
            at = 4 * (z - 1) + 2 * late
            return tuple(angles[at + k, h, pl.ds(row, TILE), :] for k in range(2))

        return turn

    def first_half(step, row, keep):
        out = advance(field, row, halves, turn_at(step, 1, row), step == 0, range(3))
        for (c, h), value in out.items():
            trial[c, h, pl.ds(row, TILE), :] = value if keep is None else value * keep

    def second_half(step, row, keep):
        last = step == SUBSTEPS - 1
        waves = (2,) if last else range(3)
        out = advance(trial, row, halves, turn_at(step + 1, 0, row), False, waves)
        for (c, h), value in out.items():
            if step > 0 or c < 4:
                value = field[c, h, pl.ds(row, TILE), :] + value
            if last:
                at = pl.multiple_of(row - begin, TILE)
                result[c - 4, h, pl.ds(at, TILE), :] = value * (UNITS[2] * 0.5**SUBSTEPS)
            else:
                field[c, h, pl.ds(row, TILE), :] = value if keep is None else value * keep

    def sweep(half, step, edges):
        count, offset = (tiles, TILE) if edges else (tiles - 2, begin)
        group = count // GROUPS

        def body(t, carry):
            for j in range(group):
                keep = None
                if edges and j == 0:
                    keep = jnp.where(t == 0, keep_first, 1.0)
                elif edges and j == group - 1:
                    keep = jnp.where(t == GROUPS - 1, keep_last, 1.0)
                half(step, pl.multiple_of(offset + (t * group + j) * TILE, TILE), keep)
            return carry

        lax.fori_loop(0, GROUPS, body, 0)

    for step in range(SUBSTEPS):
        sweep(first_half, step, True)
        sweep(second_half, step, step < SUBSTEPS - 1)

    cosine, sine_part = plate_phase(plate_ref[...])
    parts = [[], []]
    for h in range(halves):
        blocks = [result[p, h].T for p in range(2)]
        for p in range(2):
            third_ref[p, pl.ds(h, LANES, stride=halves), :] = blocks[p]
        run = PLATE // halves
        for k in range(LANES // run):
            turn = (cosine[k : k + 1], sine_part[k : k + 1])
            piece = [b[k * run : (k + 1) * run] for b in blocks]
            product = cmul(piece, turn)
            for p in range(2):
                parts[p].append(product[p])
    real, imaginary = (jnp.concatenate(p, axis=0) for p in parts)
    data = jnp.concatenate(
        [jnp.concatenate([real, imaginary], axis=1), jnp.concatenate([-imaginary, real], axis=1)],
        axis=0,
    )
    high, low = split(data)
    for copy in copies:
        copy.wait()
    spectrum = dot(high_ref[...], high) + (dot(high_ref[...], low) + dot(low_ref[...], high))
    share = spectrum.shape[0] // devices
    for d in range(devices):
        for p in range(2):
            sent_ref[d, p] = spectrum[d * share : (d + 1) * share, p * width : (p + 1) * width]


def spot_kernel(
    got_ref, third_ref, table_high_ref, table_low_ref, low_ref, high_ref, row_ref, column_ref,
    far_ref, sent_ref, third_hbm,
    sems,
):
    copies = start_copies((third_ref,), (third_hbm,), sems)
    devices, _, share, width = got_ref.shape
    columns = column_ref.shape[1]
    classes = columns // width
    first = lax.axis_index("gx") * share

    folded = []
    for p in range(2):
        pieces = []
        for k in range(classes):
            terms = [got_ref[d, p] for d in range(k, devices, classes)]
            while len(terms) > 1:
                terms = [sum(terms[i : i + 2]) for i in range(0, len(terms), 2)]
            pieces.append(terms[0])
        folded.append(jnp.concatenate(pieces, axis=1))
    position = lax.broadcasted_iota(jnp.int32, (2 * share, columns), 1)
    parity = (1 - 2 * lax.rem(position, 2)).astype(F32)

    def transform(stacked):
        high, low = split(stacked)
        both = dot(jnp.concatenate([high, low], axis=0), table_high_ref[...])
        total = both[: 2 * share] + (both[2 * share :] + dot(high, table_low_ref[...]))
        return total[:, :columns], total[:, columns:]

    cosines, sines = transform(jnp.concatenate(folded, axis=0) * parity)
    far_real = cosines[:share] + sines[share:]
    far_imaginary = cosines[share:] - sines[:share]
    far_ref[0] = far_real
    far_ref[1] = far_imaginary

    rows = low_ref.shape[1]
    own = lax.broadcasted_iota(jnp.int32, (share, rows), 1) == first + lax.broadcasted_iota(
        jnp.int32, (share, rows), 0
    )

    def own_rows(ref):
        value = jnp.where(own, ref[...].astype(F32), 0.0)
        return jnp.sum(value, axis=1, keepdims=True)

    spot = lax.broadcasted_iota(jnp.int32, (share, columns), 1).astype(F32)
    inside = (spot >= own_rows(low_ref)) & (spot < own_rows(high_ref))
    gain = own_rows(row_ref) * column_ref[...]
    power = far_real * far_real + far_imaginary * far_imaginary
    factor = jnp.where(inside, gain * lax.rsqrt(jnp.maximum(power, 1.0)), 1.0)
    replaced = jnp.concatenate([far_real * factor, far_imaginary * factor], axis=0)
    cosines, sines = transform(replaced)
    parity = parity[:share]
    across = (
        (cosines[:share] - sines[share:]) * parity,
        (cosines[share:] + sines[:share]) * parity,
    )
    for d in range(devices):
        k = d % classes
        for p in range(2):
            sent_ref[d, p] = across[p][:, k * width : (k + 1) * width]
    for copy in copies:
        copy.wait()


def back_kernel(got_ref, far_ref, plate_ref, high_ref, low_ref, back_hbm, far_hbm, back_ref, sems):
    copies = start_copies((far_ref,), (far_hbm,), sems)
    devices, _, share, width = got_ref.shape
    real = got_ref[:, 0].reshape(devices * share, width)
    imaginary = got_ref[:, 1].reshape(devices * share, width)
    data = jnp.concatenate(
        [jnp.concatenate([real, imaginary], axis=1), jnp.concatenate([imaginary, -real], axis=1)],
        axis=0,
    )
    high, low = split(data)
    total = dot(high_ref[...], high) + (dot(high_ref[...], low) + dot(low_ref[...], high))
    cosine, sine_part = plate_phase(plate_ref[...])
    for k in range(total.shape[0] // PLATE):
        rows = slice(k * PLATE, (k + 1) * PLATE)
        piece = (total[rows, :width], total[rows, width:])
        turn = (cosine[k : k + 1], sine_part[k : k + 1])
        product = cmul_conj(piece, turn)
        for p in range(2):
            back_ref[p, rows, :] = product[p]
        if k % 2:
            done = pl.ds((k - 1) * PLATE, 2 * PLATE)
            copies += start_copies(
                (back_ref.at[:, done],), (back_hbm.at[:, done],), sems.at[pl.ds(1 + k // 2, 1)]
            )
    for copy in copies:
        copy.wait()


def shape(*dims):
    return jax.ShapeDtypeStruct(dims, F32)


def away(array):
    return pltpu.with_memory_space_constraint(jnp.asarray(array), pltpu.HBM)


HELD = pl.BlockSpec(memory_space=pltpu.VMEM)
AWAY = pl.BlockSpec(memory_space=pltpu.HBM)


def call(kernel, name, inputs, outputs, scratch):
    return pl.pallas_call(
        kernel,
        in_specs=inputs,
        out_specs=[spec for spec, _ in outputs],
        out_shape=[out for _, out in outputs],
        scratch_shapes=scratch,
        compiler_params=pltpu.CompilerParams(vmem_limit_bytes=20 * 2**20),
        name=name,
    )


def local(wave_one, wave_two, mismatch, plate, spot_low, spot_high, row_gain, column_gain):
    devices = lax.axis_size("gx")
    rows, width = wave_one.shape[1:]
    far_rows, far_columns = row_gain.shape[0], column_gain.shape[0]
    whole_width = width * devices
    halves = rows // LANES
    share = far_rows // devices
    assert rows % LANES == 0 and width == LANES and PLATE % halves == 0
    assert (width // TILE) % GROUPS == 0
    assert far_columns % width == 0 and devices % (far_columns // width) == 0
    assert (whole_width // 2) % far_columns == 0 and devices % 2 == 0
    scale = FAR_SCALE / math.sqrt(rows * whole_width)
    forward, backward = row_tables(rows, far_rows, scale)
    columns = column_tables(far_columns)

    whole = shape(2, rows, width)
    strip = (HELD, shape(5, halves, HALO, LANES))
    turned, near, far = call(
        edges_kernel,
        "edges",
        [AWAY] * 3,
        [(HELD, shape(5, halves, width, LANES)), strip, strip],
        [
            pltpu.VMEM((2, rows, width), F32),
            pltpu.VMEM((2, rows, width), F32),
            pltpu.VMEM((rows, width), F32),
            pltpu.SemaphoreType.DMA((3,)),
        ],
    )(*(away(a) for a in (wave_one, wave_two, mismatch)))
    near = lax.ppermute(near, "gx", [(i, i ^ 1) for i in range(devices)])
    pairs = [(i, i + 1) for i in range(1, devices - 1, 2)]
    far = lax.ppermute(far, "gx", pairs + [(j, i) for i, j in pairs])

    length = width + 4 * TILE
    spots = [a.reshape(1, -1) for a in (spot_low, spot_high, row_gain, column_gain)]
    chunks = (HELD, shape(devices, 2, share, width))
    third, sent, *spots = call(
        crystal_kernel,
        "crystal",
        [HELD] * 4 + [AWAY] * 6,
        [(HELD, whole), chunks, *((HELD, jax.ShapeDtypeStruct(a.shape, a.dtype)) for a in spots)],
        [
            pltpu.VMEM((6, halves, length, LANES), F32),
            pltpu.VMEM((6, halves, length, LANES), F32),
            pltpu.VMEM((4 * SUBSTEPS - 2, halves, length, LANES), F32),
            pltpu.VMEM((2, halves, width, LANES), F32),
            pltpu.VMEM(forward[0].shape, BF16),
            pltpu.VMEM(forward[1].shape, BF16),
            pltpu.SemaphoreType.DMA((6,)),
        ],
    )(turned, near, far, plate, *(away(a) for a in (*forward, *spots)))
    got = lax.all_to_all(sent, "gx", 0, 0, tiled=True)
    far_field, sent, third = call(
        spot_kernel,
        "spot",
        [HELD] * 8,
        [(HELD, shape(2, share, far_columns)), chunks, (AWAY, whole)],
        [pltpu.SemaphoreType.DMA((1,))],
    )(got, third, *columns, *spots)
    got = lax.all_to_all(sent, "gx", 0, 0, tiled=True)
    back, far_field = call(
        back_kernel,
        "back",
        [HELD] * 5,
        [(AWAY, whole), (AWAY, shape(2, share, far_columns))],
        [pltpu.VMEM((2, rows, width), F32), pltpu.SemaphoreType.DMA((1 + rows // (2 * PLATE),))],
    )(got, far_field, plate, *backward)
    return third, far_field, back


def solution(mesh):
    return jax.shard_map(
        local,
        mesh=mesh,
        in_specs=(
            P(None, "groups", "gx"),
            P(None, "groups", "gx"),
            P("groups", "gx"),
            P("groups", "gx"),
            P("groups"),
            P("groups"),
            P("groups"),
            P("groups"),
        ),
        out_specs=(
            P(None, "groups", "gx"),
            P(None, ("groups", "gx"), None),
            P(None, "groups", "gx"),
        ),
        check_vma=False,
    )
```

```python
import functools
import math

import jax
import jax.numpy as jnp
import ml_dtypes
import numpy as np
from jax import lax
from jax.experimental import pallas as pl
from jax.experimental.pallas import tpu as pltpu
from jax.sharding import PartitionSpec as P

SUBSTEPS = 4
ZOOM = 4
LEVELS = 16
PLATE = 32

DIFFRACT = (0.08, 0.04, 0.027)
WALKOFF = (0.3, -0.8, 0.8)
COUPLE = (0.08, 0.16, 0.24)
FAR_SCALE = 4.0

UNITS = tuple(
    math.sqrt(COUPLE[j] / (COUPLE[0] * COUPLE[1] * COUPLE[2])) for j in range(3)
)
HALO = 2 * SUBSTEPS
TILE = 8
LANES = 128
F32 = jnp.float32
BF16 = jnp.bfloat16


def split_table(table):
    high = table.astype(np.float32).astype(ml_dtypes.bfloat16)
    low = (table - high.astype(np.float64)).astype(np.float32).astype(ml_dtypes.bfloat16)
    return high, low


def row_tables(rows, far_rows, scale):
    u = np.arange(far_rows, dtype=np.int64) - far_rows // 2
    y = np.arange(rows, dtype=np.int64) - rows // 2
    period = ZOOM * rows
    angle = 2.0 * np.pi / period * np.mod(u[:, None] * y[None, :], period)
    real, imaginary = scale * np.cos(angle), -scale * np.sin(angle)
    halves = rows // LANES
    order = np.arange(rows).reshape(LANES, halves).T.reshape(-1)
    forward = np.concatenate([real[:, order], imaginary[:, order]], axis=1)
    backward = np.concatenate([real.T, imaginary.T], axis=1)
    return split_table(forward), split_table(backward)


def column_tables(far_columns):
    v = np.arange(far_columns, dtype=np.int64)
    angle = 2.0 * np.pi / far_columns * np.mod(v[:, None] * v[None, :], far_columns)
    return split_table(np.concatenate([np.cos(angle), np.sin(angle)], axis=1))


def split(value):
    high = value.astype(BF16)
    low = (value - high.astype(F32)).astype(BF16)
    return high, low


def dot(left, right):
    return jnp.dot(left, right, preferred_element_type=F32)


def plate_phase(levels):
    count, across = levels.shape
    block = lax.broadcasted_iota(jnp.int32, (count, across * PLATE), 1) // PLATE
    level = jnp.zeros((count, across * PLATE), F32)
    for b in range(across):
        level = jnp.where(block == b, levels[:, b : b + 1].astype(F32), level)
    angle = (2.0 * math.pi / LEVELS) * level
    return jnp.cos(angle), jnp.sin(angle)


def start_copies(sources, targets, sems):
    copies = [
        pltpu.make_async_copy(a, b, sems.at[i]) for i, (a, b) in enumerate(zip(sources, targets))
    ]
    for copy in copies:
        copy.start()
    return copies


def edges_kernel(
    one_hbm, two_hbm, mismatch_hbm, turned_ref, near_ref, far_ref,
    one_ref, two_ref, mismatch_ref, sems,
):
    halves = one_ref.shape[1] // LANES
    width = one_ref.shape[2]
    copies = start_copies(
        (one_hbm, two_hbm, mismatch_hbm), (one_ref, two_ref, mismatch_ref), sems
    )
    even = lax.rem(lax.axis_index("gx"), 2) == 0
    for c in range(5):
        if c % 2 == 0:
            copies[c // 2].wait()
        for h in range(halves):
            rows = pl.ds(h, LANES, stride=halves)
            if c < 2:
                block = one_ref[c, rows, :] * (1.0 / UNITS[0])
            elif c < 4:
                block = two_ref[c - 2, rows, :] * (1.0 / UNITS[1])
            else:
                block = mismatch_ref[rows, :]
            block = block.T
            turned_ref[c, h] = block
            first, last = block[:HALO], block[width - HALO :]
            near_ref[c, h] = jnp.where(even, last, first)
            far_ref[c, h] = jnp.where(even, first, last)


def sine_pair(angle):
    q = angle * angle
    sine = (1.0 / math.factorial(13)) * q - 1.0 / math.factorial(11)
    cosine = (-1.0 / math.factorial(14)) * q + 1.0 / math.factorial(12)
    for k in (9, 7, 5, 3, 1):
        sine = sine * q + (-1.0) ** (k // 2) / math.factorial(k)
    for k in (10, 8, 6, 4, 2, 0):
        cosine = cosine * q + (-1.0) ** (k // 2) / math.factorial(k)
    return cosine, sine * angle


def cmul(a, b):
    return a[0] * b[0] - a[1] * b[1], a[0] * b[1] + a[1] * b[0]


def cmul_conj(a, b):
    return a[0] * b[0] + a[1] * b[1], a[1] * b[0] - a[0] * b[1]


def advance(source, row, halves, turn, start, waves):
    lane = lax.broadcasted_iota(jnp.int32, (TILE, LANES), 1)
    used = range(4) if start else range(6)
    mid = [[source[c, h, pl.ds(row, TILE), :] for h in range(halves)] for c in used]
    linear = {}
    for wave in waves:
        if start and wave == 2:
            continue
        side = -1 if WALKOFF[wave] > 0 else 1
        drift, spread = abs(WALKOFF[wave]), DIFFRACT[wave]
        for part in range(2):
            c = 2 * wave + part
            wrap = jnp.where(lane == 0, 0.0, pltpu.roll(mid[c][-1], 1, 1))
            over = jnp.where(lane == LANES - 1, 0.0, pltpu.roll(mid[c][0], LANES - 1, 1))
            for h in range(halves):
                above = mid[c][h - 1] if h else wrap
                below = mid[c][h + 1] if h + 1 < halves else over
                left = source[c, h, pl.ds(row - 1, TILE), :]
                right = source[c, h, pl.ds(row + 1, TILE), :]
                around = (above + below) + (left + right)
                m = mid[c][h]
                bend = spread * around - (4.0 * spread) * m
                move = (1.0 - drift) * m + drift * (left if side < 0 else right)
                linear[c, h] = (bend, move)
    out = {}
    for h in range(halves):
        a1, a2 = (mid[0][h], mid[1][h]), (mid[2][h], mid[3][h])
        mixes = {}
        if start:
            mixes[2] = cmul(a1, a2)
        else:
            a3 = (mid[4][h], mid[5][h])
            phase = turn(h)
            if 0 in waves:
                back = cmul_conj(a3, phase) if phase is not None else a3
                mixes[0] = cmul_conj(back, a2)
                mixes[1] = cmul_conj(back, a1)
            ahead = cmul(a1, phase) if phase is not None else a1
            mixes[2] = cmul(ahead, a2)
        for wave in waves:
            real, imaginary = 2 * wave, 2 * wave + 1
            mix = mixes.get(wave)
            if (real, h) not in linear:
                out[real, h], out[imaginary, h] = -mix[1], mix[0]
                continue
            real_part = linear[real, h][1] - linear[imaginary, h][0]
            imaginary_part = linear[imaginary, h][1] + linear[real, h][0]
            if mix is not None:
                real_part = real_part - mix[1]
                imaginary_part = imaginary_part + mix[0]
            out[real, h], out[imaginary, h] = real_part, imaginary_part
    return out


def store_angles(angles, h, row, value):
    c1, s1 = sine_pair(value)
    one = (c1, s1)
    two = (c1 * c1 - s1 * s1, 2.0 * c1 * s1)
    three = cmul(one, two)
    four = (two[0] * two[0] - two[1] * two[1], 2.0 * two[0] * two[1])
    for z, pair in enumerate((one, two, three, four)):
        for late in range(2 if z < 3 else 1):
            at, unit = 4 * z + 2 * late, 0.5 ** (z + late)
            for k in range(2):
                angles[at + k, h, pl.ds(row, TILE), :] = unit * pair[k]


def propagate(field, trial, angles, halves, rows, keep, store):
    def turn_at(z, late, row):
        def turn(h):
            if z == 0:
                return None
            at = 4 * (z - 1) + 2 * late
            return tuple(angles[at + k, h, pl.ds(row, TILE), :] for k in range(2))

        return turn

    for step in range(SUBSTEPS):
        last = step == SUBSTEPS - 1
        for j, row in enumerate(rows):
            waves = (2,) if last and j in (0, len(rows) - 1) else range(3)
            out = advance(field, row, halves, turn_at(step, 1, row), step == 0, waves)
            for (c, h), value in out.items():
                trial[c, h, pl.ds(row, TILE), :] = value * keep[j] if j in keep else value
        for j, row in enumerate(rows[1:-1] if last else rows):
            waves = (2,) if last else range(3)
            out = advance(trial, row, halves, turn_at(step + 1, 0, row), False, waves)
            for (c, h), value in out.items():
                if step > 0 or c < 4:
                    value = field[c, h, pl.ds(row, TILE), :] + value
                if last:
                    store(c - 4, h, row, value * (UNITS[2] * 0.5**SUBSTEPS))
                else:
                    field[c, h, pl.ds(row, TILE), :] = value * keep[j] if j in keep else value


def inner_kernel(turned_ref, near_ref, *rest):
    count = (len(rest) - 5) // 2
    away_refs, (result_ref, *held_refs) = rest[:count], rest[count : 2 * count + 1]
    field, trial, angles, sems = rest[2 * count + 1 :]
    copies = start_copies(away_refs, held_refs, sems)
    halves, width = turned_ref.shape[1], turned_ref.shape[2]
    odd = lax.rem(lax.axis_index("gx"), 2)
    count = width // TILE
    begin = 2 * TILE
    first = pl.multiple_of((2 - odd) * TILE, TILE)
    beside = pl.multiple_of(TILE + (1 - odd) * (width + TILE), TILE)

    zero = jnp.zeros((TILE, LANES), F32)
    for h in range(halves):
        for c in range(6):
            for at in (0, TILE, begin + width, begin + width + TILE):
                field[c, h, pl.ds(at, TILE), :] = zero
                trial[c, h, pl.ds(at, TILE), :] = zero
        for c in range(4):
            field[c, h, pl.ds(begin, width), :] = turned_ref[c, h]
            field[c, h, pl.ds(beside, TILE), :] = near_ref[c, h]
        store_angles(angles, h, beside, near_ref[4, h])

    def angle_body(t, carry):
        for h in range(halves):
            row = pl.multiple_of(t * TILE, TILE)
            value = turned_ref[4, h, pl.ds(row, TILE), :]
            store_angles(angles, h, pl.multiple_of(row + begin, TILE), value)
        return carry

    lax.fori_loop(0, count, angle_body, 0, unroll=4)
    rows = [pl.multiple_of(first + j * TILE, TILE) for j in range(count + 1)]

    def store(p, h, row, value):
        result_ref[p, h, pl.ds(pl.multiple_of(row - begin, TILE), TILE), :] = value

    propagate(field, trial, angles, halves, rows, {}, store)
    for copy in copies:
        copy.wait()


def outer_kernel(
    turned_ref, far_ref, inner_ref, plate_ref, high_ref, low_ref,
    third_ref, sent_ref,
    field, trial, angles, result,
):
    halves, width = turned_ref.shape[1], turned_ref.shape[2]
    devices = sent_ref.shape[0]
    index = lax.axis_index("gx")
    even = lax.rem(index, 2) == 0
    present = jnp.where((index > 0) & (index < devices - 1), 1.0, 0.0).astype(F32)
    keep = {0: jnp.where(even, present, 1.0), 2: jnp.where(even, 1.0, present)}
    rows = [TILE, 2 * TILE, 3 * TILE]

    zero = jnp.zeros((TILE, LANES), F32)
    for h in range(halves):
        for c in range(6):
            for at in (0, 4 * TILE):
                field[c, h, pl.ds(at, TILE), :] = zero
                trial[c, h, pl.ds(at, TILE), :] = zero
        for c in range(5):
            beyond = far_ref[c, h]
            low = [turned_ref[c, h, pl.ds(j * TILE, TILE), :] for j in range(2)]
            top = [turned_ref[c, h, pl.ds(width - (2 - j) * TILE, TILE), :] for j in range(2)]
            around = ((beyond, top[0]), (low[0], top[1]), (low[1], beyond))
            for j, (left, right) in enumerate(around):
                value = jnp.where(even, left, right)
                if c < 4:
                    field[c, h, pl.ds(rows[j], TILE), :] = value * keep[j] if j in keep else value
                else:
                    store_angles(angles, h, rows[j], value)
        for p in range(2):
            result[p, h] = inner_ref[p, h]
    edge = pl.multiple_of(jnp.where(even, 0, width - TILE), TILE)

    def store(p, h, row, value):
        result[p, h, pl.ds(edge, TILE), :] = value

    propagate(field, trial, angles, halves, rows, keep, store)

    cosine, sine_part = plate_phase(plate_ref[...])
    parts = [[], []]
    for h in range(halves):
        blocks = [result[p, h].T for p in range(2)]
        for p in range(2):
            third_ref[p, pl.ds(h, LANES, stride=halves), :] = blocks[p]
        run = PLATE // halves
        for k in range(LANES // run):
            turn = (cosine[k : k + 1], sine_part[k : k + 1])
            piece = [b[k * run : (k + 1) * run] for b in blocks]
            product = cmul(piece, turn)
            for p in range(2):
                parts[p].append(product[p])
    real, imaginary = (jnp.concatenate(p, axis=0) for p in parts)
    data = jnp.concatenate(
        [jnp.concatenate([real, imaginary], axis=1), jnp.concatenate([-imaginary, real], axis=1)],
        axis=0,
    )
    high, low = split(data)
    spectrum = dot(high_ref[...], high) + (dot(high_ref[...], low) + dot(low_ref[...], high))
    share = spectrum.shape[0] // devices
    for d in range(devices):
        for p in range(2):
            sent_ref[d, p] = spectrum[d * share : (d + 1) * share, p * width : (p + 1) * width]


def spot_kernel(
    got_ref, table_high_ref, table_low_ref, low_ref, high_ref, row_ref, column_ref,
    far_ref, sent_ref,
):
    devices, _, share, width = got_ref.shape
    columns = column_ref.shape[1]
    classes = columns // width
    first = lax.axis_index("gx") * share

    folded = []
    for p in range(2):
        pieces = []
        for k in range(classes):
            terms = [got_ref[d, p] for d in range(k, devices, classes)]
            while len(terms) > 1:
                terms = [sum(terms[i : i + 2]) for i in range(0, len(terms), 2)]
            pieces.append(terms[0])
        folded.append(jnp.concatenate(pieces, axis=1))
    position = lax.broadcasted_iota(jnp.int32, (2 * share, columns), 1)
    parity = (1 - 2 * lax.rem(position, 2)).astype(F32)

    def transform(stacked):
        high, low = split(stacked)
        both = dot(jnp.concatenate([high, low], axis=0), table_high_ref[...])
        total = both[: 2 * share] + (both[2 * share :] + dot(high, table_low_ref[...]))
        return total[:, :columns], total[:, columns:]

    cosines, sines = transform(jnp.concatenate(folded, axis=0) * parity)
    far_real = cosines[:share] + sines[share:]
    far_imaginary = cosines[share:] - sines[:share]
    far_ref[0] = far_real
    far_ref[1] = far_imaginary

    rows = low_ref.shape[1]
    own = lax.broadcasted_iota(jnp.int32, (share, rows), 1) == first + lax.broadcasted_iota(
        jnp.int32, (share, rows), 0
    )

    def own_rows(ref):
        value = jnp.where(own, ref[...].astype(F32), 0.0)
        return jnp.sum(value, axis=1, keepdims=True)

    spot = lax.broadcasted_iota(jnp.int32, (share, columns), 1).astype(F32)
    inside = (spot >= own_rows(low_ref)) & (spot < own_rows(high_ref))
    gain = own_rows(row_ref) * column_ref[...]
    power = far_real * far_real + far_imaginary * far_imaginary
    factor = jnp.where(inside, gain * lax.rsqrt(jnp.maximum(power, 1.0)), 1.0)
    replaced = jnp.concatenate([far_real * factor, far_imaginary * factor], axis=0)
    cosines, sines = transform(replaced)
    parity = parity[:share]
    across = (
        (cosines[:share] - sines[share:]) * parity,
        (cosines[share:] + sines[:share]) * parity,
    )
    for d in range(devices):
        k = d % classes
        for p in range(2):
            sent_ref[d, p] = across[p][:, k * width : (k + 1) * width]


def back_kernel(
    got_ref, far_ref, third_ref, plate_ref, high_ref, low_ref,
    back_hbm, far_hbm, third_hbm,
    back_ref, sems,
):
    copies = start_copies((far_ref, third_ref), (far_hbm, third_hbm), sems)
    devices, _, share, width = got_ref.shape
    real = got_ref[:, 0].reshape(devices * share, width)
    imaginary = got_ref[:, 1].reshape(devices * share, width)
    data = jnp.concatenate(
        [jnp.concatenate([real, imaginary], axis=1), jnp.concatenate([imaginary, -real], axis=1)],
        axis=0,
    )
    high, low = split(data)
    total = dot(high_ref[...], high) + (dot(high_ref[...], low) + dot(low_ref[...], high))
    cosine, sine_part = plate_phase(plate_ref[...])
    for k in range(total.shape[0] // PLATE):
        rows = slice(k * PLATE, (k + 1) * PLATE)
        piece = (total[rows, :width], total[rows, width:])
        turn = (cosine[k : k + 1], sine_part[k : k + 1])
        product = cmul_conj(piece, turn)
        for p in range(2):
            back_ref[p, rows, :] = product[p]
        if k % 2:
            done = pl.ds((k - 1) * PLATE, 2 * PLATE)
            copies += start_copies(
                (back_ref.at[:, done],), (back_hbm.at[:, done],), sems.at[pl.ds(2 + k // 2, 1)]
            )
    for copy in copies:
        copy.wait()


def shape(*dims):
    return jax.ShapeDtypeStruct(dims, F32)


def away(array):
    return pltpu.with_memory_space_constraint(jnp.asarray(array), pltpu.HBM)


HELD = pl.BlockSpec(memory_space=pltpu.VMEM)
AWAY = pl.BlockSpec(memory_space=pltpu.HBM)


def call(kernel, name, inputs, outputs, scratch):
    return pl.pallas_call(
        kernel,
        in_specs=inputs,
        out_specs=[spec for spec, _ in outputs],
        out_shape=[out for _, out in outputs],
        scratch_shapes=scratch,
        compiler_params=pltpu.CompilerParams(vmem_limit_bytes=20 * 2**20),
        name=name,
    )


def local(wave_one, wave_two, mismatch, plate, spot_low, spot_high, row_gain, column_gain):
    devices = lax.axis_size("gx")
    rows, width = wave_one.shape[1:]
    far_rows, far_columns = row_gain.shape[0], column_gain.shape[0]
    whole_width = width * devices
    halves = rows // LANES
    share = far_rows // devices
    assert rows % LANES == 0 and width == LANES and PLATE % halves == 0
    assert far_columns % width == 0 and devices % (far_columns // width) == 0
    assert (whole_width // 2) % far_columns == 0 and devices % 2 == 0
    scale = FAR_SCALE / math.sqrt(rows * whole_width)
    forward, backward = row_tables(rows, far_rows, scale)
    columns = column_tables(far_columns)

    whole = shape(2, rows, width)
    strip = (HELD, shape(5, halves, HALO, LANES))
    turned, near, far = call(
        edges_kernel,
        "edges",
        [AWAY] * 3,
        [(HELD, shape(5, halves, width, LANES)), strip, strip],
        [
            pltpu.VMEM((2, rows, width), F32),
            pltpu.VMEM((2, rows, width), F32),
            pltpu.VMEM((rows, width), F32),
            pltpu.SemaphoreType.DMA((3,)),
        ],
    )(*(away(a) for a in (wave_one, wave_two, mismatch)))
    near = lax.ppermute(near, "gx", [(i, i ^ 1) for i in range(devices)])
    pairs = [(i, i + 1) for i in range(1, devices - 1, 2)]
    far = lax.ppermute(far, "gx", pairs + [(j, i) for i, j in pairs])

    spots = [a.reshape(1, -1) for a in (spot_low, spot_high, row_gain, column_gain)]
    chunks = (HELD, shape(devices, 2, share, width))

    def planes(length):
        return [
            pltpu.VMEM((6, halves, length, LANES), F32),
            pltpu.VMEM((6, halves, length, LANES), F32),
            pltpu.VMEM((4 * SUBSTEPS - 2, halves, length, LANES), F32),
        ]

    result = shape(2, halves, width, LANES)
    fetched = (*forward, *spots)
    inner, high, low, *spots = call(
        inner_kernel,
        "inner",
        [HELD] * 2 + [AWAY] * len(fetched),
        [(HELD, result), *((HELD, jax.ShapeDtypeStruct(a.shape, a.dtype)) for a in fetched)],
        planes(width + 4 * TILE) + [pltpu.SemaphoreType.DMA((len(fetched),))],
    )(turned, near, *(away(a) for a in fetched))
    third, sent = call(
        outer_kernel,
        "outer",
        [HELD] * 6,
        [(HELD, whole), chunks],
        planes(5 * TILE) + [pltpu.VMEM(result.shape, F32)],
    )(turned, far, inner, plate, high, low)
    got = lax.all_to_all(sent, "gx", 0, 0, tiled=True)
    far_field, sent = call(
        spot_kernel,
        "spot",
        [HELD] * 7,
        [(HELD, shape(2, share, far_columns)), chunks],
        [],
    )(got, *columns, *spots)
    got = lax.all_to_all(sent, "gx", 0, 0, tiled=True)
    back, far_field, third = call(
        back_kernel,
        "back",
        [HELD] * 6,
        [(AWAY, whole), (AWAY, shape(2, share, far_columns)), (AWAY, whole)],
        [pltpu.VMEM((2, rows, width), F32), pltpu.SemaphoreType.DMA((2 + rows // (2 * PLATE),))],
    )(got, far_field, third, plate, *backward)
    return third, far_field, back


def solution(mesh):
    return jax.shard_map(
        local,
        mesh=mesh,
        in_specs=(
            P(None, "groups", "gx"),
            P(None, "groups", "gx"),
            P("groups", "gx"),
            P("groups", "gx"),
            P("groups"),
            P("groups"),
            P("groups"),
            P("groups"),
        ),
        out_specs=(
            P(None, "groups", "gx"),
            P(None, ("groups", "gx"), None),
            P(None, "groups", "gx"),
        ),
        check_vma=False,
    )
```

```python
import functools
import math

import jax
import jax.numpy as jnp
import ml_dtypes
import numpy as np
from jax import lax
from jax.experimental import pallas as pl
from jax.experimental.pallas import tpu as pltpu
from jax.sharding import PartitionSpec as P

SUBSTEPS = 4
ZOOM = 4
LEVELS = 16
PLATE = 32

DIFFRACT = (0.08, 0.04, 0.027)
WALKOFF = (0.3, -0.8, 0.8)
COUPLE = (0.08, 0.16, 0.24)
FAR_SCALE = 4.0

UNITS = tuple(
    math.sqrt(COUPLE[j] / (COUPLE[0] * COUPLE[1] * COUPLE[2])) for j in range(3)
)
HALO = 2 * SUBSTEPS
TILE = 8
LANES = 128
F32 = jnp.float32
BF16 = jnp.bfloat16


def split_table(table):
    high = table.astype(np.float32).astype(ml_dtypes.bfloat16)
    low = (table - high.astype(np.float64)).astype(np.float32).astype(ml_dtypes.bfloat16)
    return high, low


def row_tables(rows, far_rows, scale):
    u = np.arange(far_rows, dtype=np.int64) - far_rows // 2
    y = np.arange(rows, dtype=np.int64) - rows // 2
    period = ZOOM * rows
    angle = 2.0 * np.pi / period * np.mod(u[:, None] * y[None, :], period)
    real, imaginary = scale * np.cos(angle), -scale * np.sin(angle)
    halves = rows // LANES
    order = np.arange(rows).reshape(LANES, halves).T.reshape(-1)
    forward = np.concatenate([real[:, order], imaginary[:, order]], axis=1)
    backward = np.concatenate([real.T, imaginary.T], axis=1)
    return split_table(forward), split_table(backward)


def column_tables(far_columns):
    v = np.arange(far_columns, dtype=np.int64)
    angle = 2.0 * np.pi / far_columns * np.mod(v[:, None] * v[None, :], far_columns)
    return split_table(np.concatenate([np.cos(angle), np.sin(angle)], axis=1))


def split(value):
    high = value.astype(BF16)
    low = (value - high.astype(F32)).astype(BF16)
    return high, low


def dot(left, right):
    return jnp.dot(left, right, preferred_element_type=F32)


def plate_phase(levels):
    count, across = levels.shape
    shape = (count, across * PLATE)
    block = lax.broadcasted_iota(jnp.int32, shape, 1) // PLATE
    level = jnp.zeros(shape, F32)
    for b in range(across):
        level = jnp.where(block == b, levels[:, b : b + 1], level)
    angle = (2.0 * math.pi / LEVELS) * level
    return jnp.cos(angle), jnp.sin(angle)


def start_copies(sources, targets, sems):
    copies = [
        pltpu.make_async_copy(a, b, sems.at[i]) for i, (a, b) in enumerate(zip(sources, targets))
    ]
    for copy in copies:
        copy.start()
    return copies


def edges_kernel(
    one_hbm, two_hbm, mismatch_hbm, plate_hbm, turned_ref, near_ref, far_ref, phase_ref,
    one_ref, two_ref, mismatch_ref, plate_ref, sems,
):
    halves = one_ref.shape[1] // LANES
    width = one_ref.shape[2]
    copies = start_copies(
        (one_hbm, two_hbm, mismatch_hbm, plate_hbm),
        (one_ref, two_ref, mismatch_ref, plate_ref),
        sems,
    )
    even = lax.rem(lax.axis_index("gx"), 2) == 0
    for c in range(5):
        if c % 2 == 0:
            copies[c // 2].wait()
        if c == 4:
            copies[3].wait()
            phase_ref[0], phase_ref[1] = plate_phase(plate_ref[...].astype(F32).T)
        for h in range(halves):
            rows = pl.ds(h, LANES, stride=halves)
            if c < 2:
                block = one_ref[c, rows, :] * (1.0 / UNITS[0])
            elif c < 4:
                block = two_ref[c - 2, rows, :] * (1.0 / UNITS[1])
            else:
                block = mismatch_ref[rows, :]
            block = block.T
            turned_ref[c, h] = block
            first, last = block[:HALO], block[width - HALO :]
            near_ref[c, h] = jnp.where(even, last, first)
            far_ref[c, h] = jnp.where(even, first, last)


def sine_pair(angle):
    q = angle * angle
    sine = (-1.0 / math.factorial(11)) * q + 1.0 / math.factorial(9)
    cosine = (1.0 / math.factorial(12)) * q - 1.0 / math.factorial(10)
    for k in (7, 5, 3, 1):
        sine = sine * q + (-1.0) ** (k // 2) / math.factorial(k)
    for k in (8, 6, 4, 2, 0):
        cosine = cosine * q + (-1.0) ** (k // 2) / math.factorial(k)
    return cosine, sine * angle


def cmul(a, b):
    return a[0] * b[0] - a[1] * b[1], a[0] * b[1] + a[1] * b[0]


def cmul_conj(a, b):
    return a[0] * b[0] + a[1] * b[1], a[1] * b[0] - a[0] * b[1]


def advance(source, row, halves, turn, start, waves):
    lane = lax.broadcasted_iota(jnp.int32, (TILE, LANES), 1)
    used = range(4) if start else range(6)
    mid = [[source[c, h, pl.ds(row, TILE), :] for h in range(halves)] for c in used]
    linear = {}
    for wave in waves:
        if start and wave == 2:
            continue
        side = -1 if WALKOFF[wave] > 0 else 1
        drift, spread = abs(WALKOFF[wave]), DIFFRACT[wave]
        for part in range(2):
            c = 2 * wave + part
            wrap = jnp.where(lane == 0, 0.0, pltpu.roll(mid[c][-1], 1, 1))
            over = jnp.where(lane == LANES - 1, 0.0, pltpu.roll(mid[c][0], LANES - 1, 1))
            for h in range(halves):
                above = mid[c][h - 1] if h else wrap
                below = mid[c][h + 1] if h + 1 < halves else over
                left = source[c, h, pl.ds(row - 1, TILE), :]
                right = source[c, h, pl.ds(row + 1, TILE), :]
                around = (above + below) + (left + right)
                m = mid[c][h]
                bend = spread * around - (4.0 * spread) * m
                move = (1.0 - drift) * m + drift * (left if side < 0 else right)
                linear[c, h] = (bend, move)
    out = {}
    for h in range(halves):
        a1, a2 = (mid[0][h], mid[1][h]), (mid[2][h], mid[3][h])
        mixes = {}
        if start:
            mixes[2] = cmul(a1, a2)
        else:
            a3 = (mid[4][h], mid[5][h])
            phase = turn(h)
            if 0 in waves:
                back = cmul_conj(a3, phase) if phase is not None else a3
                mixes[0] = cmul_conj(back, a2)
                mixes[1] = cmul_conj(back, a1)
            ahead = cmul(a1, phase) if phase is not None else a1
            mixes[2] = cmul(ahead, a2)
        for wave in waves:
            real, imaginary = 2 * wave, 2 * wave + 1
            mix = mixes.get(wave)
            if (real, h) not in linear:
                out[real, h], out[imaginary, h] = -mix[1], mix[0]
                continue
            real_part = linear[real, h][1] - linear[imaginary, h][0]
            imaginary_part = linear[imaginary, h][1] + linear[real, h][0]
            if mix is not None:
                real_part = real_part - mix[1]
                imaginary_part = imaginary_part + mix[0]
            out[real, h], out[imaginary, h] = real_part, imaginary_part
    return out


def store_angles(angles, h, row, value):
    c1, s1 = sine_pair(value)
    one, half = (c1, s1), (0.5 * c1, 0.5 * s1)
    two = (c1 * half[0] - s1 * half[1], c1 * s1)
    two_half = (0.5 * two[0], 0.5 * two[1])
    three = cmul(two, half)
    three_half = (0.5 * three[0], 0.5 * three[1])
    four = (two[0] * two_half[0] - two[1] * two_half[1], two[0] * two[1])
    for at, pair in enumerate((one, half, two, two_half, three, three_half, four)):
        for k in range(2):
            angles[2 * at + k, h, pl.ds(row, TILE), :] = pair[k]


def propagate(field, trial, angles, halves, rows, keep, store):
    def turn_at(z, late, row):
        def turn(h):
            if z == 0:
                return None
            at = 4 * (z - 1) + 2 * late
            return tuple(angles[at + k, h, pl.ds(row, TILE), :] for k in range(2))

        return turn

    for step in range(SUBSTEPS):
        last = step == SUBSTEPS - 1
        for j, row in enumerate(rows):
            waves = (2,) if last and j in (0, len(rows) - 1) else range(3)
            out = advance(field, row, halves, turn_at(step, 1, row), step == 0, waves)
            for (c, h), value in out.items():
                trial[c, h, pl.ds(row, TILE), :] = value * keep[j] if j in keep else value
        for j, row in enumerate(rows[1:-1] if last else rows):
            waves = (2,) if last else range(3)
            out = advance(trial, row, halves, turn_at(step + 1, 0, row), False, waves)
            for (c, h), value in out.items():
                if step > 0 or c < 4:
                    value = field[c, h, pl.ds(row, TILE), :] + value
                if last:
                    store(c - 4, h, row, value * (UNITS[2] * 0.5**SUBSTEPS))
                else:
                    field[c, h, pl.ds(row, TILE), :] = value * keep[j] if j in keep else value


def inner_kernel(turned_ref, near_ref, *rest):
    count = (len(rest) - 5) // 2
    away_refs, (result_ref, *held_refs) = rest[:count], rest[count : 2 * count + 1]
    field, trial, angles, sems = rest[2 * count + 1 :]
    copies = start_copies(away_refs, held_refs, sems)
    halves, width = turned_ref.shape[1], turned_ref.shape[2]
    odd = lax.rem(lax.axis_index("gx"), 2)
    count = width // TILE
    begin = 2 * TILE
    first = pl.multiple_of((2 - odd) * TILE, TILE)
    beside = pl.multiple_of(TILE + (1 - odd) * (width + TILE), TILE)

    zero = jnp.zeros((TILE, LANES), F32)
    for h in range(halves):
        for c in range(6):
            for at in (0, TILE, begin + width, begin + width + TILE):
                field[c, h, pl.ds(at, TILE), :] = zero
                trial[c, h, pl.ds(at, TILE), :] = zero
        for c in range(4):
            field[c, h, pl.ds(begin, width), :] = turned_ref[c, h]
            field[c, h, pl.ds(beside, TILE), :] = near_ref[c, h]
        store_angles(angles, h, beside, near_ref[4, h])

    def angle_body(t, carry):
        for h in range(halves):
            row = pl.multiple_of(t * TILE, TILE)
            value = turned_ref[4, h, pl.ds(row, TILE), :]
            store_angles(angles, h, pl.multiple_of(row + begin, TILE), value)
        return carry

    lax.fori_loop(0, count, angle_body, 0, unroll=4)
    rows = [pl.multiple_of(first + j * TILE, TILE) for j in range(count + 1)]

    def store(p, h, row, value):
        result_ref[p, h, pl.ds(pl.multiple_of(row - begin, TILE), TILE), :] = value

    propagate(field, trial, angles, halves, rows, {}, store)
    for copy in copies:
        copy.wait()


def outer_kernel(
    turned_ref, far_ref, inner_ref, phase_ref, high_ref, low_ref,
    third_ref, sent_ref,
    field, trial, angles, result,
):
    halves, width = turned_ref.shape[1], turned_ref.shape[2]
    devices = sent_ref.shape[0]
    index = lax.axis_index("gx")
    even = lax.rem(index, 2) == 0
    present = jnp.where((index > 0) & (index < devices - 1), 1.0, 0.0).astype(F32)
    keep = {0: jnp.where(even, present, 1.0), 2: jnp.where(even, 1.0, present)}
    rows = [TILE, 2 * TILE, 3 * TILE]

    zero = jnp.zeros((TILE, LANES), F32)
    for h in range(halves):
        for c in range(6):
            for at in (0, 4 * TILE):
                field[c, h, pl.ds(at, TILE), :] = zero
                trial[c, h, pl.ds(at, TILE), :] = zero
        for c in range(5):
            beyond = far_ref[c, h]
            low = [turned_ref[c, h, pl.ds(j * TILE, TILE), :] for j in range(2)]
            top = [turned_ref[c, h, pl.ds(width - (2 - j) * TILE, TILE), :] for j in range(2)]
            around = ((beyond, top[0]), (low[0], top[1]), (low[1], beyond))
            for j, (left, right) in enumerate(around):
                value = jnp.where(even, left, right)
                if c < 4:
                    field[c, h, pl.ds(rows[j], TILE), :] = value * keep[j] if j in keep else value
                else:
                    store_angles(angles, h, rows[j], value)
        for p in range(2):
            result[p, h] = inner_ref[p, h]
    edge = pl.multiple_of(jnp.where(even, 0, width - TILE), TILE)

    def store(p, h, row, value):
        result[p, h, pl.ds(edge, TILE), :] = value

    propagate(field, trial, angles, halves, rows, keep, store)

    cosine, sine_part = phase_ref[0], phase_ref[1]
    parts = [[], []]
    for h in range(halves):
        blocks = [result[p, h].T for p in range(2)]
        for p in range(2):
            third_ref[p, pl.ds(h, LANES, stride=halves), :] = blocks[p]
        run = PLATE // halves
        for k in range(LANES // run):
            turn = (cosine[k : k + 1], sine_part[k : k + 1])
            piece = [b[k * run : (k + 1) * run] for b in blocks]
            product = cmul(piece, turn)
            for p in range(2):
                parts[p].append(product[p])
    real, imaginary = (jnp.concatenate(p, axis=0) for p in parts)
    data = jnp.concatenate(
        [jnp.concatenate([real, imaginary], axis=1), jnp.concatenate([-imaginary, real], axis=1)],
        axis=0,
    )
    high, low = split(data)
    spectrum = dot(high_ref[...], high) + (dot(high_ref[...], low) + dot(low_ref[...], high))
    share = spectrum.shape[0] // devices
    for d in range(devices):
        for p in range(2):
            sent_ref[d, p] = spectrum[d * share : (d + 1) * share, p * width : (p + 1) * width]


def spot_kernel(
    got_ref, table_high_ref, table_low_ref, low_ref, high_ref, row_ref, column_ref,
    far_ref, sent_ref,
):
    devices, _, share, width = got_ref.shape
    columns = column_ref.shape[1]
    classes = columns // width
    first = lax.axis_index("gx") * share

    folded = []
    for p in range(2):
        pieces = []
        for k in range(classes):
            terms = [got_ref[d, p] for d in range(k, devices, classes)]
            while len(terms) > 1:
                terms = [sum(terms[i : i + 2]) for i in range(0, len(terms), 2)]
            pieces.append(terms[0])
        folded.append(jnp.concatenate(pieces, axis=1))
    position = lax.broadcasted_iota(jnp.int32, (2 * share, columns), 1)
    parity = (1 - 2 * lax.rem(position, 2)).astype(F32)

    def transform(stacked):
        high, low = split(stacked)
        both = dot(jnp.concatenate([high, low], axis=0), table_high_ref[...])
        total = both[: 2 * share] + (both[2 * share :] + dot(high, table_low_ref[...]))
        return total[:, :columns], total[:, columns:]

    cosines, sines = transform(jnp.concatenate(folded, axis=0) * parity)
    far_real = cosines[:share] + sines[share:]
    far_imaginary = cosines[share:] - sines[:share]
    far_ref[0] = far_real
    far_ref[1] = far_imaginary

    rows = low_ref.shape[1]
    own = lax.broadcasted_iota(jnp.int32, (share, rows), 1) == first + lax.broadcasted_iota(
        jnp.int32, (share, rows), 0
    )

    def own_rows(ref):
        value = jnp.where(own, ref[...].astype(F32), 0.0)
        return jnp.sum(value, axis=1, keepdims=True)

    spot = lax.broadcasted_iota(jnp.int32, (share, columns), 1).astype(F32)
    inside = (spot >= own_rows(low_ref)) & (spot < own_rows(high_ref))
    gain = own_rows(row_ref) * column_ref[...]
    power = far_real * far_real + far_imaginary * far_imaginary
    factor = jnp.where(inside, gain * lax.rsqrt(jnp.maximum(power, 1.0)), 1.0)
    replaced = jnp.concatenate([far_real * factor, far_imaginary * factor], axis=0)
    cosines, sines = transform(replaced)
    parity = parity[:share]
    across = (
        (cosines[:share] - sines[share:]) * parity,
        (cosines[share:] + sines[:share]) * parity,
    )
    for d in range(devices):
        k = d % classes
        for p in range(2):
            sent_ref[d, p] = across[p][:, k * width : (k + 1) * width]


def back_kernel(
    got_ref, far_ref, third_ref, phase_ref, high_ref, low_ref,
    back_hbm, far_hbm, third_hbm,
    back_ref, sems,
):
    copies = start_copies((far_ref, third_ref), (far_hbm, third_hbm), sems)
    devices, _, share, width = got_ref.shape
    real = got_ref[:, 0].reshape(devices * share, width)
    imaginary = got_ref[:, 1].reshape(devices * share, width)
    data = jnp.concatenate(
        [jnp.concatenate([real, imaginary], axis=1), jnp.concatenate([imaginary, -real], axis=1)],
        axis=0,
    )
    high, low = split(data)
    total = dot(high_ref[...], high) + (dot(high_ref[...], low) + dot(low_ref[...], high))
    cosine, sine_part = phase_ref[0], phase_ref[1]
    for k in range(total.shape[0] // PLATE):
        rows = slice(k * PLATE, (k + 1) * PLATE)
        piece = (total[rows, :width], total[rows, width:])
        turn = (cosine[k : k + 1], sine_part[k : k + 1])
        product = cmul_conj(piece, turn)
        for p in range(2):
            back_ref[p, rows, :] = product[p]
        if k % 2:
            done = pl.ds((k - 1) * PLATE, 2 * PLATE)
            copies += start_copies(
                (back_ref.at[:, done],), (back_hbm.at[:, done],), sems.at[pl.ds(2 + k // 2, 1)]
            )
    for copy in copies:
        copy.wait()


def shape(*dims):
    return jax.ShapeDtypeStruct(dims, F32)


def away(array):
    return pltpu.with_memory_space_constraint(jnp.asarray(array), pltpu.HBM)


HELD = pl.BlockSpec(memory_space=pltpu.VMEM)
AWAY = pl.BlockSpec(memory_space=pltpu.HBM)


def call(kernel, name, inputs, outputs, scratch):
    return pl.pallas_call(
        kernel,
        in_specs=inputs,
        out_specs=[spec for spec, _ in outputs],
        out_shape=[out for _, out in outputs],
        scratch_shapes=scratch,
        compiler_params=pltpu.CompilerParams(vmem_limit_bytes=20 * 2**20),
        name=name,
    )


def local(wave_one, wave_two, mismatch, plate, spot_low, spot_high, row_gain, column_gain):
    devices = lax.axis_size("gx")
    rows, width = wave_one.shape[1:]
    far_rows, far_columns = row_gain.shape[0], column_gain.shape[0]
    whole_width = width * devices
    halves = rows // LANES
    share = far_rows // devices
    assert rows % LANES == 0 and width == LANES and PLATE % halves == 0
    assert far_columns % width == 0 and devices % (far_columns // width) == 0
    assert (whole_width // 2) % far_columns == 0 and devices % 2 == 0
    scale = FAR_SCALE / math.sqrt(rows * whole_width)
    forward, backward = row_tables(rows, far_rows, scale)
    columns = column_tables(far_columns)

    whole = shape(2, rows, width)
    strip = (HELD, shape(5, halves, HALO, LANES))
    turned, near, far, phase = call(
        edges_kernel,
        "edges",
        [AWAY] * 4,
        [
            (HELD, shape(5, halves, width, LANES)),
            strip,
            strip,
            (HELD, shape(2, rows // PLATE, width)),
        ],
        [
            pltpu.VMEM((2, rows, width), F32),
            pltpu.VMEM((2, rows, width), F32),
            pltpu.VMEM((rows, width), F32),
            pltpu.VMEM(plate.shape[::-1], plate.dtype),
            pltpu.SemaphoreType.DMA((4,)),
        ],
    )(*(away(a) for a in (wave_one, wave_two, mismatch, plate.T)))
    near = lax.ppermute(near, "gx", [(i, i ^ 1) for i in range(devices)])
    pairs = [(i, i + 1) for i in range(1, devices - 1, 2)]
    far = lax.ppermute(far, "gx", pairs + [(j, i) for i, j in pairs])

    spots = [a.reshape(1, -1) for a in (spot_low, spot_high, row_gain, column_gain)]
    chunks = (HELD, shape(devices, 2, share, width))

    def planes(length):
        return [
            pltpu.VMEM((6, halves, length, LANES), F32),
            pltpu.VMEM((6, halves, length, LANES), F32),
            pltpu.VMEM((4 * SUBSTEPS - 2, halves, length, LANES), F32),
        ]

    result = shape(2, halves, width, LANES)
    fetched = (*forward, *spots)
    inner, high, low, *spots = call(
        inner_kernel,
        "inner",
        [HELD] * 2 + [AWAY] * len(fetched),
        [(HELD, result), *((HELD, jax.ShapeDtypeStruct(a.shape, a.dtype)) for a in fetched)],
        planes(width + 4 * TILE) + [pltpu.SemaphoreType.DMA((len(fetched),))],
    )(turned, near, *(away(a) for a in fetched))
    third, sent = call(
        outer_kernel,
        "outer",
        [HELD] * 6,
        [(HELD, whole), chunks],
        planes(5 * TILE) + [pltpu.VMEM(result.shape, F32)],
    )(turned, far, inner, phase, high, low)
    got = lax.all_to_all(sent, "gx", 0, 0, tiled=True)
    far_field, sent = call(
        spot_kernel,
        "spot",
        [HELD] * 7,
        [(HELD, shape(2, share, far_columns)), chunks],
        [],
    )(got, *columns, *spots)
    got = lax.all_to_all(sent, "gx", 0, 0, tiled=True)
    back, far_field, third = call(
        back_kernel,
        "back",
        [HELD] * 6,
        [(AWAY, whole), (AWAY, shape(2, share, far_columns)), (AWAY, whole)],
        [pltpu.VMEM((2, rows, width), F32), pltpu.SemaphoreType.DMA((2 + rows // (2 * PLATE),))],
    )(got, far_field, third, phase, *backward)
    return third, far_field, back


def solution(mesh):
    return jax.shard_map(
        local,
        mesh=mesh,
        in_specs=(
            P(None, "groups", "gx"),
            P(None, "groups", "gx"),
            P("groups", "gx"),
            P("groups", "gx"),
            P("groups"),
            P("groups"),
            P("groups"),
            P("groups"),
        ),
        out_specs=(
            P(None, "groups", "gx"),
            P(None, ("groups", "gx"), None),
            P(None, "groups", "gx"),
        ),
        check_vma=False,
    )
```
